32 devices in a mesh: samp: 16 (over z, y, x), tp: 2 (over core).
Axes of the slice: x: 2, y: 2, z: 4, core: 2. Of those that a mesh axis runs over, the one named last changes fastest.
Arguments:
- images: bfloat16 [128, 12288], P(None, 'tp'), may hold values from -6 to 6
- enc_mean: float32 [128, 128], replicated, may hold values from -0.3 to 0.3
- enc_logscale: float32 [128, 128], replicated, may hold values from -0.15 to 0
- noise: float32 [128, 128, 128], P(None, 'samp'), may hold values from -5 to 5
- w_in: bfloat16 [128, 1024], P(None, 'tp'), may hold values from -0.5 to 0.5
- b_in: bfloat16 [1, 1024], P(None, 'tp'), may hold values from -3 to 3
- w_out: bfloat16 [1024, 12288], P(None, 'tp'), may hold values from -0.0078125 to 0.0078125
- b_out: float32 [1, 12288], P(None, 'tp'), may hold values from -3 to 3
- pixel_logscale: float32 [1, 12288], P(None, 'tp'), may hold values from 0 to 1
Outputs:
- bound: float32 [128], replicated
- log_weights: float32 [128, 128], P(None, 'samp')
The draws below stay inside these ranges and needn't reach their ends.
All inputs are finite; a program needn't handle non-finite values.
Results may differ from the reference program's by a relative error of at most 0.00073.
Values may be sent and summed in bfloat16 or wider, within the bound.
No kernel may reach another device: no remote copies, remote signals or barrier semaphores. Data moves between devices by JAX's collectives and lax.ppermute only.
A program may use at most 64 MiB of HBM per device.

```python
import math
import jax
import jax.numpy as jnp
from jax import lax

PIX = 12288
HID = 1024
LAT = 128
IMG = 128
K = 128


def draw_w_out(key, part):
    dense_key = jax.random.fold_in(key, 101)
    row_key = jax.random.fold_in(key, 202)
    column_key = jax.random.fold_in(key, 303)
    deviation = 2.5 / math.sqrt(HID * 2048)
    dense_part = jax.random.normal(dense_key, (HID, PIX), jnp.float32) * deviation
    row_factor = jax.random.normal(row_key, (HID,), jnp.float32)
    column_factor = jax.random.normal(column_key, (PIX,), jnp.float32)
    combined = dense_part + 0.5 * deviation * row_factor[:, None] * column_factor[None, :]
    return jnp.clip(combined, -0.0078125, 0.0078125).astype(jnp.bfloat16)


def block_scale(key, dims, split, least, top_value):
    def one(axis_at, shards_of):
        heights = jax.random.uniform(jax.random.fold_in(jax.random.fold_in(key, 6), axis_at), (shards_of,), jnp.float32, least / len(split), top_value / len(split))
        return jnp.repeat(jnp.exp(heights), dims[axis_at] // shards_of).reshape((-1,) + (1,) * (len(dims) - axis_at - 1))

    level = one(*split[0])
    for cut in split[1:]:
        level = level * one(*cut)
    return level


def gaussian(own_key, extent, spread, reach, split=(), held_as=jnp.bfloat16):
    level = block_scale(own_key, extent, split, -0.22, 0.18) if split else 1.0
    result = jax.random.normal(own_key, extent, jnp.float32) * spread * level
    return jnp.minimum(jnp.maximum(result, -reach), reach).astype(held_as)


def setup_inputs(seed: int = 0) -> dict:
    keys = jax.random.split(jax.random.key(seed), 10)
    return {
        "images": gaussian(keys[0], (IMG, PIX), 1.0, 6.0, ((1, 2),)),
        "enc_mean": gaussian(keys[1], (IMG, LAT), 0.05, 0.3, (), jnp.float32),
        "enc_logscale": jnp.clip(jax.random.uniform(keys[2], (IMG, LAT), jnp.float32, -0.15, 0.0), -0.15, 0.0),
        "noise": gaussian(keys[3], (IMG, K, LAT), 1.0, 5.0, ((1, 16),), jnp.float32),
        "w_in": gaussian(keys[4], (LAT, HID), LAT ** -0.5, 0.5, ((1, 2),)),
        "b_in": gaussian(keys[5], (1, HID), 0.5, 3.0, ((1, 2),)),
        "w_out": draw_w_out(jax.random.fold_in(keys[9], 71), 0),
        "b_out": gaussian(keys[7], (1, PIX), 0.5, 3.0, ((1, 2),), jnp.float32),
        "pixel_logscale": jnp.clip(1.0 * jax.random.uniform(keys[8], (1, PIX), jnp.float32) ** block_scale(keys[8], (1, PIX), ((1, 2),), -0.2, 0.2), 0.0, 1.0),
    }


HALF_LOG_TAU = 0.9189385332046727


def reference(images, enc_mean, enc_logscale, noise, w_in, b_in, w_out, b_out, pixel_logscale):
    latent = enc_mean[:, None, :] + jnp.exp(enc_logscale)[:, None, :] * noise
    inverse = jnp.exp(-pixel_logscale)
    constant = -jnp.sum(pixel_logscale) - PIX * HALF_LOG_TAU

    def image_loglik(operands):
        latent_one, image_one = operands
        latent_rows = latent_one.astype(jnp.bfloat16)
        hidden = jax.nn.relu(jnp.dot(latent_rows, w_in, preferred_element_type=jnp.float32) + b_in.astype(jnp.float32)).astype(jnp.bfloat16)
        pixel_mean = jnp.dot(hidden, w_out, preferred_element_type=jnp.float32) + b_out
        scaled = (image_one[None, :].astype(jnp.float32) - pixel_mean) * inverse
        return jnp.sum(-0.5 * scaled * scaled, axis=1)

    loglik = lax.map(image_loglik, (latent, images)) + constant
    prior = jnp.sum(-0.5 * latent * latent - HALF_LOG_TAU, axis=2)
    posterior = jnp.sum(-0.5 * noise * noise - enc_logscale[:, None, :] - HALF_LOG_TAU, axis=2)
    logw = loglik + prior - posterior
    peak = jnp.max(logw, axis=1)
    sum_exp = jnp.sum(jnp.exp(logw - peak[:, None]), axis=1)
    bound = (peak + jnp.log(sum_exp) - jnp.log(jnp.float32(K))) / PIX
    log_weights = (logw - peak[:, None]) - jnp.log(sum_exp)[:, None] + jnp.log(jnp.float32(K))
    return bound, log_weights
```

```python
import functools
import math

import jax
import jax.numpy as jnp
from jax import lax
from jax.experimental import pallas as pl
from jax.experimental.pallas import tpu as pltpu
from jax.sharding import PartitionSpec as P

HALF_LOG_TAU = 0.9189385332046727


def decoder_kernel(
    row_chunk,
    tp_size,
    noise_ref,
    mean_ref,
    logscale_ref,
    w_in_ref,
    b_in_ref,
    w_ref,
    bias_ref,
    pixel_logscale_ref,
    image_ref,
    whole_logscale_ref,
    out_ref,
    hidden_ref,
    squares_ref,
    latent_terms_ref,
):
    step = pl.program_id(0)
    images, samples, latent_dims = noise_ref.shape
    rows = images * samples
    width = w_ref.shape[1]

    @pl.when(step == 0)
    def _():
        noise = noise_ref[...]
        logscale = logscale_ref[...][:, None, :]
        latent = mean_ref[...][:, None, :] + jnp.exp(logscale) * noise
        latent_terms_ref[...] = (
            (-0.5 * latent * latent) - (-0.5 * noise * noise - logscale)
        ) * (1.0 / tp_size)
        squares_ref[...] = jnp.zeros_like(squares_ref)
        latent_rows = latent.reshape(rows, latent_dims).astype(jnp.bfloat16)
        hidden = jnp.dot(latent_rows, w_in_ref[...], preferred_element_type=jnp.float32)
        hidden = hidden + b_in_ref[...].astype(jnp.float32)
        hidden_ref[...] = jnp.maximum(hidden, 0.0).astype(jnp.bfloat16)

    inverse = jnp.exp(-pixel_logscale_ref[...])
    target = (image_ref[...].astype(jnp.float32) - bias_ref[...]) * inverse
    image_chunk = row_chunk // samples
    for at in range(0, rows, row_chunk):
        first = at // samples
        mean = jnp.dot(
            hidden_ref[at : at + row_chunk, :], w_ref[...], preferred_element_type=jnp.float32
        ).reshape(image_chunk, samples, width)
        scaled = target[first : first + image_chunk, None, :] - mean * inverse[None]
        square = scaled * scaled
        folded = square[:, :, :128]
        for lane in range(128, width, 128):
            folded = folded + square[:, :, lane : lane + 128]
        squares_ref[first : first + image_chunk] += folded

    @pl.when(step == pl.num_programs(0) - 1)
    def _():
        constant = -jnp.sum(whole_logscale_ref[...]) - whole_logscale_ref.shape[1] * HALF_LOG_TAU
        terms = latent_terms_ref[...] - 0.5 * squares_ref[...]
        sums = jnp.sum(terms, axis=2, keepdims=True)
        image_at = lax.broadcasted_iota(jnp.int32, (images, samples, images), 0)
        lane_at = lax.broadcasted_iota(jnp.int32, (images, samples, images), 2)
        placed = jnp.sum(jnp.where(image_at == lane_at, sums, 0.0), axis=0) + constant
        out_ref[...] = jnp.broadcast_to(placed[None], out_ref.shape)


def finish_kernel(samp_axis, tp_size, all_pixels, received_ref, bound_ref, weights_ref):
    samp_size = received_ref.shape[0] // tp_size
    samples = received_ref.shape[1]
    all_samples = samp_size * samples
    parts = received_ref[...].reshape(samp_size, tp_size, *received_ref.shape[1:])
    logw = parts[:, 0]
    for half in range(1, tp_size):
        logw = logw + parts[:, half]
    peak = jnp.max(jnp.max(logw, axis=0), axis=0, keepdims=True)
    sum_exp = jnp.sum(jnp.sum(jnp.exp(logw - peak[None]), axis=0), axis=0, keepdims=True)
    log_sum = jnp.log(sum_exp)
    log_count = math.log(all_samples)
    bound_ref[...] = (peak + log_sum - log_count) / all_pixels
    me = lax.axis_index(samp_axis)
    own = received_ref[pl.ds(me * tp_size, tp_size)]
    mine = own[0]
    for half in range(1, tp_size):
        mine = mine + own[half]
    weights_ref[...] = (mine - peak) - log_sum + log_count


def on_device(
    mesh_shape, images, enc_mean, enc_logscale, noise, w_in, b_in, w_out, b_out, pixel_logscale
):
    samp_size, tp_size = mesh_shape["samp"], mesh_shape["tp"]
    devices = samp_size * tp_size
    image_count, sample_count, latent_dims = noise.shape
    rows = image_count * sample_count
    hidden_units = w_out.shape[0]
    share = images.shape[1]
    width = math.gcd(share, 1024)
    w_whole, b_whole = (
        lax.all_gather(w_in, "tp", axis=1, tiled=True),
        lax.all_gather(b_in, "tp", axis=1, tiled=True),
    )
    whole = lambda shape: pl.BlockSpec(shape, lambda j: (0,) * len(shape))
    columns = lambda count: pl.BlockSpec((count, width), lambda j: (0, j))
    partial = pl.pallas_call(
        functools.partial(decoder_kernel, math.gcd(rows, 256), tp_size),
        grid=(share // width,),
        in_specs=[
            whole(noise.shape),
            whole(enc_mean.shape),
            whole(enc_logscale.shape),
            whole(w_whole.shape),
            whole(b_whole.shape),
            columns(hidden_units),
            columns(1),
            columns(1),
            columns(image_count),
            whole(pixel_logscale.shape),
        ],
        out_specs=whole((devices, sample_count, image_count)),
        out_shape=jax.ShapeDtypeStruct((devices, sample_count, image_count), jnp.float32),
        scratch_shapes=[
            pltpu.VMEM((rows, hidden_units), jnp.bfloat16),
            pltpu.VMEM((image_count, sample_count, 128), jnp.float32),
            pltpu.VMEM((image_count, sample_count, latent_dims), jnp.float32),
        ],
        cost_estimate=pl.CostEstimate(
            flops=2 * rows * hidden_units * (share + latent_dims),
            bytes_accessed=2 * hidden_units * share + 2 * image_count * share + 4 * rows * latent_dims,
            transcendentals=share,
        ),
        name="decoder",
    )(
        noise,
        enc_mean,
        enc_logscale,
        w_whole,
        b_whole,
        w_out,
        b_out,
        pixel_logscale,
        images,
        pixel_logscale,
    )
    received = lax.all_to_all(partial, ("samp", "tp"), 0, 0)
    bound, weights = pl.pallas_call(
        functools.partial(finish_kernel, "samp", tp_size, share * tp_size),
        out_shape=(
            jax.ShapeDtypeStruct((1, image_count), jnp.float32),
            jax.ShapeDtypeStruct((sample_count, image_count), jnp.float32),
        ),
        name="finish",
    )(received)
    return bound.reshape(image_count), weights.T


def solution(mesh):
    in_specs = (
        P(None, "tp"),
        P(),
        P(),
        P(None, "samp", None),
        P(None, "tp"),
        P(None, "tp"),
        P(None, "tp"),
        P(None, "tp"),
        P(None, "tp"),
    )
    out_specs = (P(), P(None, "samp"))
    return jax.shard_map(
        functools.partial(on_device, dict(mesh.shape)),
        mesh=mesh,
        in_specs=in_specs,
        out_specs=out_specs,
        check_vma=False,
    )
```

```python
import functools
import math

import jax
import jax.numpy as jnp
from jax import lax
from jax.experimental import pallas as pl
from jax.experimental.pallas import tpu as pltpu
from jax.sharding import PartitionSpec as P

HALF_LOG_TAU = 0.9189385332046727
TILE = 256
LANES = 128


def w_block(w_hbm, target, sem, tp_axis, tp_size, block):
    units, width = w_hbm.shape[0] // tp_size, target.shape[1]
    me = lax.axis_index(tp_axis)
    copies = []
    for part in range(tp_size):
        owner = lax.rem(me + tp_size - part, tp_size)
        copies.append(
            pltpu.make_async_copy(
                w_hbm.at[
                    pl.ds(pl.multiple_of(owner * units, units), units),
                    pl.ds(pl.multiple_of(block * width, width), width),
                ],
                target.at[pl.ds(part * units, units), :],
                sem.at[part],
            )
        )
    return copies


def prepare_kernel(
    tp_axis,
    tp_size,
    noise_hbm,
    mean_hbm,
    logscale_hbm,
    w_in_hbm,
    b_in_hbm,
    bias_hbm,
    pixel_logscale_hbm,
    image_hbm,
    w_hbm,
    latent_ref,
    hidden_ref,
    prior_ref,
    target_ref,
    inverse_ref,
    head_ref,
    noise_ref,
    mean_ref,
    logscale_ref,
    w_in_ref,
    b_in_ref,
    bias_ref,
    pixel_logscale_ref,
    image_ref,
    sem,
    head_sem,
):
    samples, images, latent_dims = noise_ref.shape
    blocks, _, width = target_ref.shape
    pairs = [(noise_hbm.at[:, s, :], noise_ref.at[s]) for s in range(samples)] + [
        (mean_hbm, mean_ref),
        (logscale_hbm, logscale_ref),
        (w_in_hbm, w_in_ref),
        (b_in_hbm, b_in_ref),
        (pixel_logscale_hbm, pixel_logscale_ref),
        (bias_hbm, bias_ref),
        (image_hbm, image_ref),
    ]
    copies = [pltpu.make_async_copy(a, b, sem.at[i]) for i, (a, b) in enumerate(pairs)]
    head = w_block(w_hbm, head_ref.at[0], head_sem, tp_axis, tp_size, 0)
    for copy in copies + head:
        copy.start()
    for copy in copies[: samples + 5]:
        copy.wait()

    latent_ref[:, latent_dims:] = jnp.zeros(
        (samples * images, TILE - latent_dims), jnp.bfloat16
    )
    logscale = logscale_ref[...]
    scale = jnp.exp(logscale)
    constant = (
        -jnp.sum(pixel_logscale_ref[...]) - pixel_logscale_ref.shape[1] * HALF_LOG_TAU
    )
    for s in range(samples):
        rows = slice(s * images, (s + 1) * images)
        noise = noise_ref[s]
        latent = mean_ref[...] + scale * noise
        terms = ((-0.5 * latent * latent) - (-0.5 * noise * noise - logscale)) * (
            1.0 / tp_size
        )
        prior_ref[s : s + 1, :] = jnp.sum(terms.T, axis=0, keepdims=True) + constant
        latent_b = latent.astype(jnp.bfloat16)
        latent_ref[rows, :latent_dims] = latent_b
        own = jnp.dot(latent_b, w_in_ref[...], preferred_element_type=jnp.float32)
        own = own + b_in_ref[...].astype(jnp.float32)
        hidden_ref[rows, :] = jnp.maximum(own, 0.0).astype(jnp.bfloat16)
    inverse_ref[...] = jnp.broadcast_to(
        jnp.exp(-pixel_logscale_ref[...]), inverse_ref.shape
    )
    for copy in copies[samples + 5 :]:
        copy.wait()
    for block in range(blocks):
        columns = slice(block * width, (block + 1) * width)
        target_ref[block] = (
            image_ref[:, columns].astype(jnp.float32) - bias_ref[:, columns]
        ) * inverse_ref[:1, columns]
    for copy in head:
        copy.wait()


def decoder_kernel(
    tp_axis,
    tp_size,
    latent_ref,
    own_ref,
    prior_ref,
    target_ref,
    inverse_ref,
    head_ref,
    *refs,
):
    w_in_refs, b_in_refs = refs[: tp_size - 1], refs[tp_size - 1 : 2 * tp_size - 2]
    w_hbm, out_ref, hidden_ref, w_ref, squares_ref, w_in_pad_ref, sem = refs[2 * tp_size - 2 :]
    blocks, images, width = target_ref.shape
    samples = squares_ref.shape[0]
    units = own_ref.shape[1]
    latent_dims = w_in_refs[0].shape[0]
    depth = w_hbm.shape[0] // TILE

    def w_copies(block):
        return w_block(w_hbm, w_ref.at[block - 1], sem.at[block - 1], tp_axis, tp_size, block)

    for block in range(1, blocks):
        for copy in w_copies(block):
            copy.start()

    def body(*accs):
        acc = (accs[:samples], accs[samples:])
        rows = [slice(s * images, (s + 1) * images) for s in range(samples)]
        for q in range(2):
            for s in range(samples):
                pltpu.matmul_pop(acc[q][s])

        for part in range(1, tp_size):
            w_in_pad_ref[:latent_dims, :] = w_in_refs[part - 1][...]
            w_in_pad_ref[latent_dims:, :] = jnp.zeros(
                (TILE - latent_dims, units), jnp.bfloat16
            )
            for tile in range(0, units // TILE, 2):
                for q in range(2):
                    at = (tile + q) * TILE
                    pltpu.matmul_push_rhs(
                        w_in_pad_ref[:, at : at + TILE], staging_register=1, mxu_index=q
                    )
                for s in range(samples):
                    for q in range(2):
                        pltpu.matmul_acc_lhs(
                            acc[q][s],
                            latent_ref[rows[s], :],
                            load_staged_rhs=1 if s == 0 else None,
                        )
                for s in range(samples):
                    for q in range(2):
                        at = (tile + q) * TILE
                        bias = b_in_refs[part - 1][:, at : at + TILE].astype(jnp.float32)
                        unit = jnp.maximum(pltpu.matmul_pop(acc[q][s]) + bias, 0.0)
                        at += (part - 1) * units
                        hidden_ref[rows[s], at : at + TILE] = unit.astype(jnp.bfloat16)

        def lhs(s, k):
            at = k * TILE
            if at < units:
                return own_ref[rows[s], at : at + TILE]
            return hidden_ref[rows[s], at - units : at - units + TILE]

        def push(block, k, register):
            for q in range(2):
                deep, wide = slice(k * TILE, (k + 1) * TILE), slice(q * TILE, (q + 1) * TILE)
                if isinstance(block, int) and block == 0:
                    tile = head_ref[0, deep, wide]
                else:
                    tile = w_ref[block - 1, deep, wide]
                pltpu.matmul_push_rhs(tile, staging_register=register, mxu_index=q)

        def take(block, s):
            total = squares_ref[s]
            for q in range(2):
                product = pltpu.matmul_pop(acc[q][s]).reshape(images // 8, 8, TILE)
                at = block * width + q * TILE
                if not isinstance(block, int):
                    at = pl.multiple_of(at, TILE)
                inverse = inverse_ref[:, pl.ds(at, TILE)]
                target = target_ref[block, :, q * TILE : (q + 1) * TILE]
                scaled = target.reshape(images // 8, 8, TILE) - product * inverse[None]
                square = (scaled * scaled).reshape(images, TILE)
                for lane in range(0, TILE, LANES):
                    total = total + square[:, lane : lane + LANES]
            squares_ref[s] = total

        first, second = range(samples // 2), range(samples // 2, samples)

        def half(block, mine, following, taken, done):
            for k in range(depth):
                for index, s in enumerate(mine):
                    for q in range(2):
                        pltpu.matmul_acc_lhs(
                            acc[q][s], lhs(s, k), load_staged_rhs=k % 2 if index == 0 else None
                        )
                    if index == 0:
                        if k + 1 < depth:
                            push(block, k + 1, (k + 1) % 2)
                        elif following is not None:
                            push(following, 0, 0)
                count = len(done)
                for s in done[k * count // depth : (k + 1) * count // depth]:
                    take(taken, s)

        def block_step(block):
            for copy in w_copies(block + 1):
                copy.wait()
            half(block, second, block + 1, block, first)
            half(block + 1, first, block + 1, block, second)

        squares_ref[...] = jnp.zeros_like(squares_ref)
        push(0, 0, 0)
        half(0, first, 0, None, ())
        block_step(0)

        @pl.loop(1, blocks - 1)
        def _(block):
            block_step(block)

        half(blocks - 1, second, None, blocks - 1, first)
        for s in second:
            take(blocks - 1, s)

        for s in range(samples):
            row = prior_ref[s : s + 1, :] - 0.5 * jnp.sum(
                squares_ref[s].T, axis=0, keepdims=True
            )
            out_ref[:, s, :] = jnp.broadcast_to(row, (out_ref.shape[0], images))

    pl.run_scoped(
        body,
        *[
            pltpu.ACC(q)((images, TILE), jnp.float32)
            for q in range(2)
            for _ in range(samples)
        ],
    )


def finish_kernel(samp_axis, tp_size, all_pixels, received_ref, bound_ref, weights_ref):
    samp_size = received_ref.shape[0] // tp_size
    samples = received_ref.shape[1]
    all_samples = samp_size * samples
    parts = received_ref[...].reshape(samp_size, tp_size, *received_ref.shape[1:])
    logw = parts[:, 0]
    for half in range(1, tp_size):
        logw = logw + parts[:, half]
    peak = jnp.max(jnp.max(logw, axis=0), axis=0, keepdims=True)
    sum_exp = jnp.sum(jnp.sum(jnp.exp(logw - peak[None]), axis=0), axis=0, keepdims=True)
    log_sum = jnp.log(sum_exp)
    log_count = math.log(all_samples)
    bound_ref[...] = (peak + log_sum - log_count) / all_pixels
    me = lax.axis_index(samp_axis)
    own = received_ref[pl.ds(me * tp_size, tp_size)]
    mine = own[0]
    for half in range(1, tp_size):
        mine = mine + own[half]
    weights_ref[...] = (mine - peak) - log_sum + log_count


def on_device(
    mesh_shape, images, enc_mean, enc_logscale, noise, w_in, b_in, w_out, b_out, pixel_logscale
):
    samp_size, tp_size = mesh_shape["samp"], mesh_shape["tp"]
    devices = samp_size * tp_size
    image_count, sample_count, latent_dims = noise.shape
    rows = image_count * sample_count
    units = w_in.shape[1]
    hidden_units, pixels = w_out.shape
    width = 2 * TILE
    blocks = pixels // width

    def from_neighbour(value, shift):
        return lax.ppermute(
            value, "tp", [(a, (a + shift) % tp_size) for a in range(tp_size)]
        )

    w_in_others = [from_neighbour(w_in, shift) for shift in range(1, tp_size)]
    b_in_others = [from_neighbour(b_in, shift) for shift in range(1, tp_size)]
    hbm = pl.BlockSpec(memory_space=pltpu.HBM)
    vmem = pl.BlockSpec(memory_space=pltpu.VMEM)
    f32, bf16 = jnp.float32, jnp.bfloat16
    in_hbm = lambda value: pltpu.with_memory_space_constraint(value, pltpu.HBM)
    prepared = pl.pallas_call(
        functools.partial(prepare_kernel, "tp", tp_size),
        in_specs=[hbm] * 9,
        out_specs=[vmem] * 6,
        out_shape=[
            jax.ShapeDtypeStruct((rows, TILE), bf16),
            jax.ShapeDtypeStruct((rows, units), bf16),
            jax.ShapeDtypeStruct((sample_count, image_count), f32),
            jax.ShapeDtypeStruct((blocks, image_count, width), f32),
            jax.ShapeDtypeStruct((8, pixels), f32),
            jax.ShapeDtypeStruct((1, hidden_units, width), bf16),
        ],
        scratch_shapes=[
            pltpu.VMEM((sample_count, image_count, latent_dims), f32),
            pltpu.VMEM(enc_mean.shape, f32),
            pltpu.VMEM(enc_logscale.shape, f32),
            pltpu.VMEM(w_in.shape, bf16),
            pltpu.VMEM(b_in.shape, bf16),
            pltpu.VMEM(b_out.shape, f32),
            pltpu.VMEM(pixel_logscale.shape, f32),
            pltpu.VMEM(images.shape, bf16),
            pltpu.SemaphoreType.DMA((sample_count + 7,)),
            pltpu.SemaphoreType.DMA((tp_size,)),
        ],
        compiler_params=pltpu.CompilerParams(vmem_limit_bytes=14 << 20),
        cost_estimate=pl.CostEstimate(
            flops=2 * rows * latent_dims * units + 20 * image_count * pixels,
            bytes_accessed=2 * image_count * pixels + 4 * rows * latent_dims,
            transcendentals=pixels,
        ),
        name="prepare",
    )(*map(in_hbm, (noise, enc_mean, enc_logscale, w_in, b_in, b_out, pixel_logscale, images, w_out)))
    partial = pl.pallas_call(
        functools.partial(decoder_kernel, "tp", tp_size),
        in_specs=[vmem] * (6 + 2 * (tp_size - 1)) + [hbm],
        out_specs=vmem,
        out_shape=jax.ShapeDtypeStruct((devices, sample_count, image_count), f32),
        scratch_shapes=[
            pltpu.VMEM((rows, hidden_units - units), bf16),
            pltpu.VMEM((blocks - 1, hidden_units, width), bf16),
            pltpu.VMEM((sample_count, image_count, LANES), f32),
            pltpu.VMEM((TILE, units), bf16),
            pltpu.SemaphoreType.DMA((blocks - 1, tp_size)),
        ],
        compiler_params=pltpu.CompilerParams(vmem_limit_bytes=32 << 20),
        cost_estimate=pl.CostEstimate(
            flops=2 * rows * hidden_units * pixels,
            bytes_accessed=2 * hidden_units * pixels,
            transcendentals=0,
        ),
        name="decoder",
    )(*prepared, *w_in_others, *b_in_others, in_hbm(w_out))
    received = lax.all_to_all(partial, ("samp", "tp"), 0, 0)
    bound, weights = pl.pallas_call(
        functools.partial(finish_kernel, "samp", tp_size, pixels * tp_size),
        in_specs=[vmem],
        out_shape=(
            jax.ShapeDtypeStruct((1, image_count), f32),
            jax.ShapeDtypeStruct((sample_count, image_count), f32),
        ),
        compiler_params=pltpu.CompilerParams(vmem_limit_bytes=4 << 20),
        name="finish",
    )(received)
    return bound.reshape(image_count), weights.T


def solution(mesh):
    in_specs = (
        P(None, "tp"),
        P(),
        P(),
        P(None, "samp", None),
        P(None, "tp"),
        P(None, "tp"),
        P(None, "tp"),
        P(None, "tp"),
        P(None, "tp"),
    )
    out_specs = (P(), P(None, "samp"))
    return jax.shard_map(
        functools.partial(on_device, dict(mesh.shape)),
        mesh=mesh,
        in_specs=in_specs,
        out_specs=out_specs,
        check_vma=False,
    )
```

```python
import functools
import math

import jax
import jax.numpy as jnp
from jax import lax
from jax.experimental import pallas as pl
from jax.experimental.pallas import tpu as pltpu
from jax.sharding import PartitionSpec as P

HALF_LOG_TAU = 0.9189385332046727
TILE = 256
AHEAD = 2
LANES = 128


def w_block(w_hbm, target, sem, tp_axis, tp_size, block):
    units, width = w_hbm.shape[0] // tp_size, target.shape[1]
    me = lax.axis_index(tp_axis)
    copies = []
    for part in range(tp_size):
        owner = lax.rem(me + tp_size - part, tp_size)
        copies.append(
            pltpu.make_async_copy(
                w_hbm.at[
                    pl.ds(pl.multiple_of(owner * units, units), units),
                    pl.ds(pl.multiple_of(block * width, width), width),
                ],
                target.at[pl.ds(part * units, units), :],
                sem.at[part],
            )
        )
    return copies


def prepare_kernel(
    tp_axis,
    tp_size,
    noise_hbm,
    mean_hbm,
    logscale_hbm,
    w_in_hbm,
    b_in_hbm,
    bias_hbm,
    pixel_logscale_hbm,
    image_hbm,
    w_hbm,
    latent_ref,
    hidden_ref,
    prior_ref,
    target_ref,
    inverse_ref,
    bias_ref,
    head_ref,
    noise_ref,
    mean_ref,
    logscale_ref,
    w_in_ref,
    b_in_ref,
    pixel_logscale_ref,
    image_ref,
    sem,
    head_sem,
):
    samples, images, latent_dims = noise_ref.shape
    heads, _, width = target_ref.shape
    pairs = [(noise_hbm.at[:, s, :], noise_ref.at[s]) for s in range(samples)] + [
        (mean_hbm, mean_ref),
        (logscale_hbm, logscale_ref),
        (w_in_hbm, w_in_ref),
        (b_in_hbm, b_in_ref),
        (pixel_logscale_hbm, pixel_logscale_ref),
        (bias_hbm, bias_ref),
        (image_hbm.at[:, pl.ds(0, heads * width)], image_ref),
    ]
    copies = [pltpu.make_async_copy(a, b, sem.at[i]) for i, (a, b) in enumerate(pairs)]
    head = []
    for block in range(heads):
        head += w_block(
            w_hbm, head_ref.at[block], head_sem.at[block], tp_axis, tp_size, block
        )
    for copy in copies + head:
        copy.start()
    for copy in copies[: samples + 2]:
        copy.wait()

    latent_ref[:, latent_dims:] = jnp.zeros(
        (samples * images, TILE - latent_dims), jnp.bfloat16
    )
    logscale = logscale_ref[...]
    scale = jnp.exp(logscale)
    for copy in copies[samples + 2 : samples + 5]:
        copy.wait()
    constant = (
        -jnp.sum(pixel_logscale_ref[...]) - pixel_logscale_ref.shape[1] * HALF_LOG_TAU
    )
    for s in range(samples):
        rows = slice(s * images, (s + 1) * images)
        noise = noise_ref[s]
        latent = mean_ref[...] + scale * noise
        terms = ((-0.5 * latent * latent) - (-0.5 * noise * noise - logscale)) * (
            1.0 / tp_size
        )
        prior_ref[s : s + 1, :] = jnp.sum(terms.T, axis=0, keepdims=True) + constant
        latent_b = latent.astype(jnp.bfloat16)
        latent_ref[rows, :latent_dims] = latent_b
        own = jnp.dot(latent_b, w_in_ref[...], preferred_element_type=jnp.float32)
        own = own + b_in_ref[...].astype(jnp.float32)
        hidden_ref[rows, :] = jnp.maximum(own, 0.0).astype(jnp.bfloat16)
    inverse_ref[...] = jnp.broadcast_to(
        jnp.exp(-pixel_logscale_ref[...]), inverse_ref.shape
    )
    for copy in copies[samples + 5 :]:
        copy.wait()
    for block in range(heads):
        columns = slice(block * width, (block + 1) * width)
        target_ref[block] = (
            image_ref[:, columns].astype(jnp.float32) - bias_ref[:, columns]
        ) * inverse_ref[:1, columns]
    for copy in head:
        copy.wait()


def decoder_kernel(
    tp_axis,
    tp_size,
    latent_ref,
    own_ref,
    prior_ref,
    head_target_ref,
    inverse_ref,
    bias_ref,
    head_ref,
    *refs,
):
    w_in_refs, b_in_refs = refs[: tp_size - 1], refs[tp_size - 1 : 2 * tp_size - 2]
    (
        image_hbm,
        w_hbm,
        out_ref,
        hidden_ref,
        w_ref,
        image_ref,
        target_ref,
        squares_ref,
        row_ref,
        w_in_pad_ref,
        sem,
        image_sem,
    ) = refs[2 * tp_size - 2 :]
    heads, images, width = head_target_ref.shape
    blocks = heads + w_ref.shape[0]
    samples = squares_ref.shape[0]
    units = own_ref.shape[1]
    latent_dims = w_in_refs[0].shape[0]
    depth = w_hbm.shape[0] // TILE

    def fetches(block):
        at = block - heads
        image = pltpu.make_async_copy(
            image_hbm.at[:, pl.ds(pl.multiple_of(block * width, width), width)],
            image_ref.at[at], image_sem.at[at]
        )
        w_copies = w_block(w_hbm, w_ref.at[at], sem.at[at], tp_axis, tp_size, block)
        return w_copies + [image]

    def start(block):
        for copy in fetches(block):
            copy.start()

    for block in range(heads, min(heads + AHEAD, blocks)):
        start(block)

    def body(*accs):
        acc = (accs[:samples], accs[samples:])
        rows = [slice(s * images, (s + 1) * images) for s in range(samples)]
        for q in range(2):
            for s in range(samples):
                pltpu.matmul_pop(acc[q][s])

        for part in range(1, tp_size):
            w_in_pad_ref[:latent_dims, :] = w_in_refs[part - 1][...]
            w_in_pad_ref[latent_dims:, :] = jnp.zeros(
                (TILE - latent_dims, units), jnp.bfloat16
            )
            for tile in range(0, units // TILE, 2):
                for q in range(2):
                    at = (tile + q) * TILE
                    pltpu.matmul_push_rhs(
                        w_in_pad_ref[:, at : at + TILE], staging_register=1, mxu_index=q
                    )
                for s in range(samples):
                    for q in range(2):
                        pltpu.matmul_acc_lhs(
                            acc[q][s],
                            latent_ref[rows[s], :],
                            load_staged_rhs=1 if s == 0 else None,
                        )
                for s in range(samples):
                    for q in range(2):
                        at = (tile + q) * TILE
                        bias = b_in_refs[part - 1][:, at : at + TILE].astype(jnp.float32)
                        unit = jnp.maximum(pltpu.matmul_pop(acc[q][s]) + bias, 0.0)
                        at += (part - 1) * units
                        hidden_ref[rows[s], at : at + TILE] = unit.astype(jnp.bfloat16)

        def lhs(s, k):
            at = k * TILE
            if at < units:
                return own_ref[rows[s], at : at + TILE]
            return hidden_ref[rows[s], at - units : at - units + TILE]

        def in_head(block):
            return isinstance(block, int) and block < heads

        def push(block, k):
            for q in range(2):
                deep, wide = slice(k * TILE, (k + 1) * TILE), slice(q * TILE, (q + 1) * TILE)
                if in_head(block):
                    tile = head_ref[block, deep, wide]
                else:
                    tile = w_ref[block - heads, deep, wide]
                pltpu.matmul_push_rhs(tile, staging_register=k % 2, mxu_index=q)

        def columns_of(block, first_column, count):
            at = block * width + first_column
            return pl.ds(at if isinstance(block, int) else pl.multiple_of(at, count), count)

        def make_target(block):
            columns = columns_of(block, 0, width)
            image = image_ref[block - heads].astype(jnp.float32)
            target_ref[block - heads] = (image - bias_ref[:, columns]) * inverse_ref[:1, columns]

        def finish_row(s, total):
            lanes = jnp.sum(total.T, axis=0, keepdims=True)
            row_ref[s : s + 1, :] = prior_ref[s : s + 1, :] - 0.5 * lanes

        def take(block, s):
            total = squares_ref[s]
            for q in range(2):
                product = pltpu.matmul_pop(acc[q][s]).reshape(images // 8, 8, TILE)
                inverse = inverse_ref[:, columns_of(block, q * TILE, TILE)]
                wide = slice(q * TILE, (q + 1) * TILE)
                if in_head(block):
                    target = head_target_ref[block, :, wide]
                else:
                    target = target_ref[block - heads, :, wide]
                scaled = target.reshape(images // 8, 8, TILE) - product * inverse[None]
                square = (scaled * scaled).reshape(images, TILE)
                for lane in range(0, TILE, LANES):
                    total = total + square[:, lane : lane + LANES]
            if isinstance(block, int) and block == blocks - 1:
                finish_row(s, total)
            else:
                squares_ref[s] = total

        middle = depth // 2
        first, second = range(samples // 2), range(samples // 2, samples)

        def multiply(block, mine, depths, following, taken, done):
            for k in depths:
                for index, s in enumerate(mine):
                    for q in range(2):
                        pltpu.matmul_acc_lhs(
                            acc[q][s], lhs(s, k), load_staged_rhs=k % 2 if index == 0 else None
                        )
                    if index == 0:
                        if k + 1 < depth:
                            push(block, k + 1)
                        else:
                            push(following, 0)
                count = len(done)
                for s in done[k * count // depth : (k + 1) * count // depth]:
                    take(taken, s)

        def block_step(block):
            if not in_head(block + 1):
                for copy in fetches(block + 1):
                    copy.wait()
                following = block + 1 + AHEAD
                if isinstance(block, int):
                    if following < blocks:
                        start(following)
                else:
                    pl.when(following < blocks)(functools.partial(start, following))
                make_target(block + 1)
            multiply(block, second, range(middle, depth), block + 1, block, first)
            multiply(block + 1, first, range(depth), block + 1, block, second)
            multiply(block + 1, second, range(middle), None, block + 1, first)

        squares_ref[...] = jnp.zeros_like(squares_ref)
        push(0, 0)
        multiply(0, first, range(depth), 0, 0, ())
        multiply(0, second, range(middle), None, 0, first)
        for block in range(heads):
            block_step(block)

        @pl.loop(heads, blocks - 1)
        def _(block):
            block_step(block)

        last = blocks - 1
        done = middle * len(first) // depth
        left = first[done:]
        for index, s in enumerate(second):
            for k in range(middle, depth):
                for q in range(2):
                    pltpu.matmul_acc_lhs(acc[q][s], lhs(s, k), load_staged_rhs=k % 2)
                if k + 1 < depth:
                    push(last, k + 1)
                elif s != second[-1]:
                    push(last, middle)
            if index < len(left):
                take(last, left[index])
            if index > 0:
                take(last, second[index - 1])
        for s in first[:done]:
            finish_row(s, squares_ref[s])
        take(last, second[-1])
        out_ref[...] = jnp.broadcast_to(row_ref[...][None], out_ref.shape)

    pl.run_scoped(
        body,
        *[
            pltpu.ACC(q)((images, TILE), jnp.float32)
            for q in range(2)
            for _ in range(samples)
        ],
    )


def finish_kernel(samp_axis, tp_size, all_pixels, received_ref, bound_ref, weights_ref):
    samp_size = received_ref.shape[0] // tp_size
    samples = received_ref.shape[1]
    all_samples = samp_size * samples
    parts = received_ref[...].reshape(samp_size, tp_size, *received_ref.shape[1:])
    logw = parts[:, 0]
    for half in range(1, tp_size):
        logw = logw + parts[:, half]
    peak = jnp.max(jnp.max(logw, axis=0), axis=0, keepdims=True)
    sum_exp = jnp.sum(jnp.sum(jnp.exp(logw - peak[None]), axis=0), axis=0, keepdims=True)
    log_sum = jnp.log(sum_exp)
    log_count = math.log(all_samples)
    bound_ref[...] = (peak + log_sum - log_count) / all_pixels
    me = lax.axis_index(samp_axis)
    own = received_ref[pl.ds(me * tp_size, tp_size)]
    mine = own[0]
    for half in range(1, tp_size):
        mine = mine + own[half]
    weights_ref[...] = (mine - peak) - log_sum + log_count


def on_device(
    mesh_shape, images, enc_mean, enc_logscale, noise, w_in, b_in, w_out, b_out, pixel_logscale
):
    samp_size, tp_size = mesh_shape["samp"], mesh_shape["tp"]
    devices = samp_size * tp_size
    image_count, sample_count, latent_dims = noise.shape
    rows = image_count * sample_count
    units = w_in.shape[1]
    hidden_units, pixels = w_out.shape
    width = 2 * TILE
    blocks = pixels // width
    heads = min(2, blocks - 1)

    def from_neighbour(value, shift):
        return lax.ppermute(
            value, "tp", [(a, (a + shift) % tp_size) for a in range(tp_size)]
        )

    w_in_others = [from_neighbour(w_in, shift) for shift in range(1, tp_size)]
    b_in_others = [from_neighbour(b_in, shift) for shift in range(1, tp_size)]
    hbm = pl.BlockSpec(memory_space=pltpu.HBM)
    vmem = pl.BlockSpec(memory_space=pltpu.VMEM)
    f32, bf16 = jnp.float32, jnp.bfloat16
    in_hbm = lambda value: pltpu.with_memory_space_constraint(value, pltpu.HBM)
    prepared = pl.pallas_call(
        functools.partial(prepare_kernel, "tp", tp_size),
        in_specs=[hbm] * 9,
        out_specs=[vmem] * 7,
        out_shape=[
            jax.ShapeDtypeStruct((rows, TILE), bf16),
            jax.ShapeDtypeStruct((rows, units), bf16),
            jax.ShapeDtypeStruct((sample_count, image_count), f32),
            jax.ShapeDtypeStruct((heads, image_count, width), f32),
            jax.ShapeDtypeStruct((8, pixels), f32),
            jax.ShapeDtypeStruct(b_out.shape, f32),
            jax.ShapeDtypeStruct((heads, hidden_units, width), bf16),
        ],
        scratch_shapes=[
            pltpu.VMEM((sample_count, image_count, latent_dims), f32),
            pltpu.VMEM(enc_mean.shape, f32),
            pltpu.VMEM(enc_logscale.shape, f32),
            pltpu.VMEM(w_in.shape, bf16),
            pltpu.VMEM(b_in.shape, bf16),
            pltpu.VMEM(pixel_logscale.shape, f32),
            pltpu.VMEM((image_count, heads * width), bf16),
            pltpu.SemaphoreType.DMA((sample_count + 7,)),
            pltpu.SemaphoreType.DMA((heads, tp_size)),
        ],
        compiler_params=pltpu.CompilerParams(vmem_limit_bytes=14 << 20),
        cost_estimate=pl.CostEstimate(
            flops=2 * rows * latent_dims * units + 20 * image_count * pixels,
            bytes_accessed=2 * image_count * pixels + 4 * rows * latent_dims,
            transcendentals=pixels,
        ),
        name="prepare",
    )(*map(in_hbm, (noise, enc_mean, enc_logscale, w_in, b_in, b_out, pixel_logscale, images, w_out)))
    partial = pl.pallas_call(
        functools.partial(decoder_kernel, "tp", tp_size),
        in_specs=[vmem] * (7 + 2 * (tp_size - 1)) + [hbm] * 2,
        out_specs=vmem,
        out_shape=jax.ShapeDtypeStruct((devices, sample_count, image_count), f32),
        scratch_shapes=[
            pltpu.VMEM((rows, hidden_units - units), bf16),
            pltpu.VMEM((blocks - heads, hidden_units, width), bf16),
            pltpu.VMEM((blocks - heads, image_count, width), bf16),
            pltpu.VMEM((blocks - heads, image_count, width), f32),
            pltpu.VMEM((sample_count, image_count, LANES), f32),
            pltpu.VMEM((sample_count, image_count), f32),
            pltpu.VMEM((TILE, units), bf16),
            pltpu.SemaphoreType.DMA((blocks - heads, tp_size)),
            pltpu.SemaphoreType.DMA((blocks - heads,)),
        ],
        compiler_params=pltpu.CompilerParams(vmem_limit_bytes=32 << 20),
        cost_estimate=pl.CostEstimate(
            flops=2 * rows * hidden_units * pixels,
            bytes_accessed=2 * hidden_units * pixels,
            transcendentals=0,
        ),
        name="decoder",
    )(*prepared, *w_in_others, *b_in_others, in_hbm(images), in_hbm(w_out))
    received = lax.all_to_all(partial, ("samp", "tp"), 0, 0)
    bound, weights = pl.pallas_call(
        functools.partial(finish_kernel, "samp", tp_size, pixels * tp_size),
        in_specs=[vmem],
        out_shape=(
            jax.ShapeDtypeStruct((1, image_count), f32),
            jax.ShapeDtypeStruct((sample_count, image_count), f32),
        ),
        compiler_params=pltpu.CompilerParams(vmem_limit_bytes=4 << 20),
        name="finish",
    )(received)
    return bound.reshape(image_count), weights.T


def solution(mesh):
    in_specs = (
        P(None, "tp"),
        P(),
        P(),
        P(None, "samp", None),
        P(None, "tp"),
        P(None, "tp"),
        P(None, "tp"),
        P(None, "tp"),
        P(None, "tp"),
    )
    out_specs = (P(), P(None, "samp"))
    return jax.shard_map(
        functools.partial(on_device, dict(mesh.shape)),
        mesh=mesh,
        in_specs=in_specs,
        out_specs=out_specs,
        check_vma=False,
    )
```

```python
import functools
import math

import jax
import jax.numpy as jnp
from jax import lax
from jax.experimental import pallas as pl
from jax.experimental.pallas import tpu as pltpu
from jax.sharding import PartitionSpec as P

HALF_LOG_TAU = 0.9189385332046727
TILE = 256
AHEAD = 2
LANES = 128


def w_block(w_hbm, target, sem, tp_axis, tp_size, block):
    units, width = w_hbm.shape[0] // tp_size, target.shape[1]
    me = lax.axis_index(tp_axis)
    copies = []
    for part in range(tp_size):
        owner = lax.rem(me + tp_size - part, tp_size)
        copies.append(
            pltpu.make_async_copy(
                w_hbm.at[
                    pl.ds(pl.multiple_of(owner * units, units), units),
                    pl.ds(pl.multiple_of(block * width, width), width),
                ],
                target.at[pl.ds(part * units, units), :],
                sem.at[part],
            )
        )
    return copies


def prepare_kernel(
    tp_axis,
    tp_size,
    noise_hbm,
    mean_hbm,
    logscale_hbm,
    w_in_hbm,
    b_in_hbm,
    bias_hbm,
    pixel_logscale_hbm,
    w_hbm,
    latent_ref,
    hidden_ref,
    prior_ref,
    inverse_ref,
    bias_ref,
    head_ref,
    noise_ref,
    mean_ref,
    logscale_ref,
    w_in_ref,
    b_in_ref,
    pixel_logscale_ref,
    sem,
    head_sem,
):
    samples, images, latent_dims = noise_ref.shape
    heads, _, width = head_ref.shape
    pairs = [(noise_hbm.at[:, s, :], noise_ref.at[s]) for s in range(samples)] + [
        (mean_hbm, mean_ref),
        (logscale_hbm, logscale_ref),
        (w_in_hbm, w_in_ref),
        (b_in_hbm, b_in_ref),
        (pixel_logscale_hbm, pixel_logscale_ref),
        (bias_hbm, bias_ref),
    ]
    copies = [pltpu.make_async_copy(a, b, sem.at[i]) for i, (a, b) in enumerate(pairs)]
    head = []
    for block in range(heads):
        head += w_block(
            w_hbm, head_ref.at[block], head_sem.at[block], tp_axis, tp_size, block
        )
    for copy in copies + head:
        copy.start()
    for copy in copies[: samples + 2]:
        copy.wait()

    latent_ref[:, latent_dims:] = jnp.zeros(
        (samples * images, TILE - latent_dims), jnp.bfloat16
    )
    logscale = logscale_ref[...]
    scale = jnp.exp(logscale)
    for copy in copies[samples + 2 : samples + 5]:
        copy.wait()
    constant = (
        -jnp.sum(pixel_logscale_ref[...]) - pixel_logscale_ref.shape[1] * HALF_LOG_TAU
    )
    for s in range(samples):
        rows = slice(s * images, (s + 1) * images)
        noise = noise_ref[s]
        latent = mean_ref[...] + scale * noise
        terms = ((-0.5 * latent * latent) - (-0.5 * noise * noise - logscale)) * (
            1.0 / tp_size
        )
        prior_ref[s : s + 1, :] = jnp.sum(terms.T, axis=0, keepdims=True) + constant
        latent_b = latent.astype(jnp.bfloat16)
        latent_ref[rows, :latent_dims] = latent_b
        own = jnp.dot(latent_b, w_in_ref[...], preferred_element_type=jnp.float32)
        own = own + b_in_ref[...].astype(jnp.float32)
        hidden_ref[rows, :] = jnp.maximum(own, 0.0).astype(jnp.bfloat16)
    inverse_ref[...] = jnp.broadcast_to(
        jnp.exp(-pixel_logscale_ref[...]), inverse_ref.shape
    )
    for copy in copies[samples + 5 :]:
        copy.wait()
    for copy in head:
        copy.wait()


def decoder_kernel(
    tp_axis,
    tp_size,
    latent_ref,
    own_ref,
    prior_ref,
    inverse_ref,
    bias_ref,
    head_ref,
    *refs,
):
    w_in_refs, b_in_refs = refs[: tp_size - 1], refs[tp_size - 1 : 2 * tp_size - 2]
    (
        image_ref,
        w_hbm,
        out_ref,
        hidden_ref,
        w_ref,
        target_ref,
        squares_ref,
        row_ref,
        w_in_pad_ref,
        sem,
    ) = refs[2 * tp_size - 2 :]
    heads, _, width = head_ref.shape
    blocks, images, _ = target_ref.shape
    samples = squares_ref.shape[0]
    units = own_ref.shape[1]
    latent_dims = w_in_refs[0].shape[0]
    depth = w_hbm.shape[0] // TILE

    def fetches(block):
        at = block - heads
        return w_block(w_hbm, w_ref.at[at], sem.at[at], tp_axis, tp_size, block)

    def start(block):
        for copy in fetches(block):
            copy.start()

    for block in range(heads, min(heads + AHEAD, blocks)):
        start(block)

    def body(*accs):
        acc = (accs[:samples], accs[samples:])
        rows = [slice(s * images, (s + 1) * images) for s in range(samples)]
        for q in range(2):
            for s in range(samples):
                pltpu.matmul_pop(acc[q][s])

        for part in range(1, tp_size):
            w_in_pad_ref[:latent_dims, :] = w_in_refs[part - 1][...]
            w_in_pad_ref[latent_dims:, :] = jnp.zeros(
                (TILE - latent_dims, units), jnp.bfloat16
            )
            for tile in range(0, units // TILE, 2):
                for q in range(2):
                    at = (tile + q) * TILE
                    pltpu.matmul_push_rhs(
                        w_in_pad_ref[:, at : at + TILE], staging_register=1, mxu_index=q
                    )
                for s in range(samples):
                    for q in range(2):
                        pltpu.matmul_acc_lhs(
                            acc[q][s],
                            latent_ref[rows[s], :],
                            load_staged_rhs=1 if s == 0 else None,
                        )
                for s in range(samples):
                    for q in range(2):
                        at = (tile + q) * TILE
                        bias = b_in_refs[part - 1][:, at : at + TILE].astype(jnp.float32)
                        unit = jnp.maximum(pltpu.matmul_pop(acc[q][s]) + bias, 0.0)
                        at += (part - 1) * units
                        hidden_ref[rows[s], at : at + TILE] = unit.astype(jnp.bfloat16)

        def lhs(s, k):
            at = k * TILE
            if at < units:
                return own_ref[rows[s], at : at + TILE]
            return hidden_ref[rows[s], at - units : at - units + TILE]

        def in_head(block):
            return isinstance(block, int) and block < heads

        def push(block, k):
            for q in range(2):
                deep, wide = slice(k * TILE, (k + 1) * TILE), slice(q * TILE, (q + 1) * TILE)
                if in_head(block):
                    tile = head_ref[block, deep, wide]
                else:
                    tile = w_ref[block - heads, deep, wide]
                pltpu.matmul_push_rhs(tile, staging_register=k % 2, mxu_index=q)

        def columns_of(block, first_column, count):
            at = block * width + first_column
            return pl.ds(at if isinstance(block, int) else pl.multiple_of(at, count), count)

        def make_target(block):
            columns = columns_of(block, 0, width)
            image = image_ref[:, columns].astype(jnp.float32)
            target_ref[block] = (image - bias_ref[:, columns]) * inverse_ref[:1, columns]

        def finish_row(s, total):
            lanes = jnp.sum(total.T, axis=0, keepdims=True)
            row_ref[s : s + 1, :] = prior_ref[s : s + 1, :] - 0.5 * lanes

        def take(block, s):
            total = squares_ref[s]
            for q in range(2):
                product = pltpu.matmul_pop(acc[q][s]).reshape(images // 8, 8, TILE)
                inverse = inverse_ref[:, columns_of(block, q * TILE, TILE)]
                wide = slice(q * TILE, (q + 1) * TILE)
                target = target_ref[block, :, wide]
                scaled = target.reshape(images // 8, 8, TILE) - product * inverse[None]
                square = (scaled * scaled).reshape(images, TILE)
                for lane in range(0, TILE, LANES):
                    total = total + square[:, lane : lane + LANES]
            if isinstance(block, int) and block == blocks - 1:
                finish_row(s, total)
            else:
                squares_ref[s] = total

        middle = depth // 2
        first, second = range(samples // 2), range(samples // 2, samples)

        def multiply(block, mine, depths, following, taken, done):
            for k in depths:
                for index, s in enumerate(mine):
                    for q in range(2):
                        pltpu.matmul_acc_lhs(
                            acc[q][s], lhs(s, k), load_staged_rhs=k % 2 if index == 0 else None
                        )
                    if index == 0:
                        if k + 1 < depth:
                            push(block, k + 1)
                        else:
                            push(following, 0)
                count = len(done)
                for s in done[k * count // depth : (k + 1) * count // depth]:
                    take(taken, s)

        def block_step(block):
            if not in_head(block + 1):
                for copy in fetches(block + 1):
                    copy.wait()
                following = block + 1 + AHEAD
                if isinstance(block, int):
                    if following < blocks:
                        start(following)
                else:
                    pl.when(following < blocks)(functools.partial(start, following))
            make_target(block + 1)
            multiply(block, second, range(middle, depth), block + 1, block, first)
            multiply(block + 1, first, range(depth), block + 1, block, second)
            multiply(block + 1, second, range(middle), None, block + 1, first)

        squares_ref[...] = jnp.zeros_like(squares_ref)
        push(0, 0)
        make_target(0)
        multiply(0, first, range(depth), 0, 0, ())
        multiply(0, second, range(middle), None, 0, first)
        for block in range(heads):
            block_step(block)

        @pl.loop(heads, blocks - 1)
        def _(block):
            block_step(block)

        last = blocks - 1
        done = middle * len(first) // depth
        left = first[done:]
        for index, s in enumerate(second):
            for k in range(middle, depth):
                for q in range(2):
                    pltpu.matmul_acc_lhs(acc[q][s], lhs(s, k), load_staged_rhs=k % 2)
                if k + 1 < depth:
                    push(last, k + 1)
                elif s != second[-1]:
                    push(last, middle)
            if index < len(left):
                take(last, left[index])
            if index > 0:
                take(last, second[index - 1])
        for s in first[:done]:
            finish_row(s, squares_ref[s])
        take(last, second[-1])
        out_ref[...] = jnp.broadcast_to(row_ref[...][None], out_ref.shape)

    pl.run_scoped(
        body,
        *[
            pltpu.ACC(q)((images, TILE), jnp.float32)
            for q in range(2)
            for _ in range(samples)
        ],
    )


def finish_kernel(samp_axis, tp_size, all_pixels, received_ref, bound_ref, weights_ref):
    samp_size = received_ref.shape[0] // tp_size
    samples = received_ref.shape[1]
    all_samples = samp_size * samples
    parts = received_ref[...].reshape(samp_size, tp_size, *received_ref.shape[1:])
    logw = parts[:, 0]
    for half in range(1, tp_size):
        logw = logw + parts[:, half]
    peak = jnp.max(jnp.max(logw, axis=0), axis=0, keepdims=True)
    sum_exp = jnp.sum(jnp.sum(jnp.exp(logw - peak[None]), axis=0), axis=0, keepdims=True)
    log_sum = jnp.log(sum_exp)
    log_count = math.log(all_samples)
    bound_ref[...] = (peak + log_sum - log_count) / all_pixels
    me = lax.axis_index(samp_axis)
    own = received_ref[pl.ds(me * tp_size, tp_size)]
    mine = own[0]
    for half in range(1, tp_size):
        mine = mine + own[half]
    weights_ref[...] = (mine - peak) - log_sum + log_count


def on_device(
    mesh_shape, images, enc_mean, enc_logscale, noise, w_in, b_in, w_out, b_out, pixel_logscale
):
    samp_size, tp_size = mesh_shape["samp"], mesh_shape["tp"]
    devices = samp_size * tp_size
    image_count, sample_count, latent_dims = noise.shape
    rows = image_count * sample_count
    units = w_in.shape[1]
    hidden_units, pixels = w_out.shape
    width = 2 * TILE
    blocks = pixels // width
    heads = min(2, blocks - 1)

    def from_neighbour(value, shift):
        return lax.ppermute(
            value, "tp", [(a, (a + shift) % tp_size) for a in range(tp_size)]
        )

    w_in_others = [from_neighbour(w_in, shift) for shift in range(1, tp_size)]
    b_in_others = [from_neighbour(b_in, shift) for shift in range(1, tp_size)]
    hbm = pl.BlockSpec(memory_space=pltpu.HBM)
    vmem = pl.BlockSpec(memory_space=pltpu.VMEM)
    f32, bf16 = jnp.float32, jnp.bfloat16
    in_hbm = lambda value: pltpu.with_memory_space_constraint(value, pltpu.HBM)
    prepared = pl.pallas_call(
        functools.partial(prepare_kernel, "tp", tp_size),
        in_specs=[hbm] * 8,
        out_specs=[vmem] * 6,
        out_shape=[
            jax.ShapeDtypeStruct((rows, TILE), bf16),
            jax.ShapeDtypeStruct((rows, units), bf16),
            jax.ShapeDtypeStruct((sample_count, image_count), f32),
            jax.ShapeDtypeStruct((8, pixels), f32),
            jax.ShapeDtypeStruct(b_out.shape, f32),
            jax.ShapeDtypeStruct((heads, hidden_units, width), bf16),
        ],
        scratch_shapes=[
            pltpu.VMEM((sample_count, image_count, latent_dims), f32),
            pltpu.VMEM(enc_mean.shape, f32),
            pltpu.VMEM(enc_logscale.shape, f32),
            pltpu.VMEM(w_in.shape, bf16),
            pltpu.VMEM(b_in.shape, bf16),
            pltpu.VMEM(pixel_logscale.shape, f32),
            pltpu.SemaphoreType.DMA((sample_count + 6,)),
            pltpu.SemaphoreType.DMA((heads, tp_size)),
        ],
        compiler_params=pltpu.CompilerParams(vmem_limit_bytes=14 << 20),
        cost_estimate=pl.CostEstimate(
            flops=2 * rows * latent_dims * units + 20 * image_count * pixels,
            bytes_accessed=2 * image_count * pixels + 4 * rows * latent_dims,
            transcendentals=pixels,
        ),
        name="prepare",
    )(*map(in_hbm, (noise, enc_mean, enc_logscale, w_in, b_in, b_out, pixel_logscale, w_out)))
    partial = pl.pallas_call(
        functools.partial(decoder_kernel, "tp", tp_size),
        in_specs=[vmem] * (7 + 2 * (tp_size - 1)) + [hbm],
        out_specs=vmem,
        out_shape=jax.ShapeDtypeStruct((devices, sample_count, image_count), f32),
        scratch_shapes=[
            pltpu.VMEM((rows, hidden_units - units), bf16),
            pltpu.VMEM((blocks - heads, hidden_units, width), bf16),
            pltpu.VMEM((blocks, image_count, width), f32),
            pltpu.VMEM((sample_count, image_count, LANES), f32),
            pltpu.VMEM((sample_count, image_count), f32),
            pltpu.VMEM((TILE, units), bf16),
            pltpu.SemaphoreType.DMA((blocks - heads, tp_size)),
        ],
        compiler_params=pltpu.CompilerParams(vmem_limit_bytes=32 << 20),
        cost_estimate=pl.CostEstimate(
            flops=2 * rows * hidden_units * pixels,
            bytes_accessed=2 * hidden_units * pixels,
            transcendentals=0,
        ),
        name="decoder",
    )(*prepared, *w_in_others, *b_in_others, images, in_hbm(w_out))
    received = lax.all_to_all(partial, ("samp", "tp"), 0, 0)
    bound, weights = pl.pallas_call(
        functools.partial(finish_kernel, "samp", tp_size, pixels * tp_size),
        in_specs=[vmem],
        out_shape=(
            jax.ShapeDtypeStruct((1, image_count), f32),
            jax.ShapeDtypeStruct((sample_count, image_count), f32),
        ),
        compiler_params=pltpu.CompilerParams(vmem_limit_bytes=4 << 20),
        name="finish",
    )(received)
    return bound.reshape(image_count), weights.T


def solution(mesh):
    in_specs = (
        P(None, "tp"),
        P(),
        P(),
        P(None, "samp", None),
        P(None, "tp"),
        P(None, "tp"),
        P(None, "tp"),
        P(None, "tp"),
        P(None, "tp"),
    )
    out_specs = (P(), P(None, "samp"))
    return jax.shard_map(
        functools.partial(on_device, dict(mesh.shape)),
        mesh=mesh,
        in_specs=in_specs,
        out_specs=out_specs,
        check_vma=False,
    )
```

```python
import functools
import math

import jax
import jax.numpy as jnp
from jax import lax
from jax.experimental import pallas as pl
from jax.experimental.pallas import tpu as pltpu
from jax.sharding import PartitionSpec as P

HALF_LOG_TAU = 0.9189385332046727
TILE = 256
AHEAD = 2
LANES = 128


def w_block(w_hbm, target, sem, tp_axis, tp_size, block):
    units, width = w_hbm.shape[0] // tp_size, target.shape[1]
    me = lax.axis_index(tp_axis)
    copies = []
    for part in range(tp_size):
        owner = lax.rem(me + tp_size - part, tp_size)
        copies.append(
            pltpu.make_async_copy(
                w_hbm.at[
                    pl.ds(pl.multiple_of(owner * units, units), units),
                    pl.ds(pl.multiple_of(block * width, width), width),
                ],
                target.at[pl.ds(part * units, units), :],
                sem.at[part],
            )
        )
    return copies


def prepare_kernel(
    tp_axis,
    tp_size,
    noise_hbm,
    mean_hbm,
    logscale_hbm,
    w_in_hbm,
    b_in_hbm,
    pixel_logscale_hbm,
    w_hbm,
    latent_ref,
    hidden_ref,
    prior_ref,
    inverse_ref,
    head_ref,
    noise_ref,
    mean_ref,
    logscale_ref,
    w_in_ref,
    b_in_ref,
    pixel_logscale_ref,
    sem,
    head_sem,
):
    samples, images, latent_dims = noise_ref.shape
    heads, _, width = head_ref.shape
    pairs = [(noise_hbm.at[:, s, :], noise_ref.at[s]) for s in range(samples)] + [
        (mean_hbm, mean_ref),
        (logscale_hbm, logscale_ref),
        (w_in_hbm, w_in_ref),
        (b_in_hbm, b_in_ref),
        (pixel_logscale_hbm, pixel_logscale_ref),
    ]
    copies = [pltpu.make_async_copy(a, b, sem.at[i]) for i, (a, b) in enumerate(pairs)]
    head = []
    for block in range(heads):
        head += w_block(
            w_hbm, head_ref.at[block], head_sem.at[block], tp_axis, tp_size, block
        )
    for copy in copies + head:
        copy.start()
    for copy in copies[: samples + 2]:
        copy.wait()

    latent_ref[:, latent_dims:] = jnp.zeros(
        (samples * images, TILE - latent_dims), jnp.bfloat16
    )
    logscale = logscale_ref[...]
    scale = jnp.exp(logscale)
    for copy in copies[samples + 2 : samples + 5]:
        copy.wait()
    constant = (
        -jnp.sum(pixel_logscale_ref[...]) - pixel_logscale_ref.shape[1] * HALF_LOG_TAU
    )
    for s in range(samples):
        rows = slice(s * images, (s + 1) * images)
        noise = noise_ref[s]
        latent = mean_ref[...] + scale * noise
        terms = ((-0.5 * latent * latent) - (-0.5 * noise * noise - logscale)) * (
            1.0 / tp_size
        )
        prior_ref[s : s + 1, :] = jnp.sum(terms.T, axis=0, keepdims=True) + constant
        latent_b = latent.astype(jnp.bfloat16)
        latent_ref[rows, :latent_dims] = latent_b
        own = jnp.dot(latent_b, w_in_ref[...], preferred_element_type=jnp.float32)
        own = own + b_in_ref[...].astype(jnp.float32)
        hidden_ref[rows, :] = jnp.maximum(own, 0.0).astype(jnp.bfloat16)
    inverse_ref[...] = jnp.broadcast_to(
        jnp.exp(-pixel_logscale_ref[...]), inverse_ref.shape
    )
    for copy in head:
        copy.wait()


def decoder_kernel(
    tp_axis,
    tp_size,
    latent_ref,
    own_ref,
    prior_ref,
    inverse_ref,
    bias_ref,
    head_ref,
    *refs,
):
    w_in_refs, b_in_refs = refs[: tp_size - 1], refs[tp_size - 1 : 2 * tp_size - 2]
    (
        image_ref,
        w_hbm,
        out_ref,
        hidden_ref,
        w_ref,
        target_ref,
        squares_ref,
        row_ref,
        w_in_pad_ref,
        sem,
    ) = refs[2 * tp_size - 2 :]
    heads, _, width = head_ref.shape
    blocks, images, _ = target_ref.shape
    samples = squares_ref.shape[0]
    units = own_ref.shape[1]
    latent_dims = w_in_refs[0].shape[0]
    depth = w_hbm.shape[0] // TILE

    def fetches(block):
        at = block - heads
        return w_block(w_hbm, w_ref.at[at], sem.at[at], tp_axis, tp_size, block)

    def start(block):
        for copy in fetches(block):
            copy.start()

    for block in range(heads, min(heads + AHEAD, blocks)):
        start(block)

    def body(*accs):
        acc = (accs[:samples], accs[samples:])
        rows = [slice(s * images, (s + 1) * images) for s in range(samples)]
        for q in range(2):
            for s in range(samples):
                pltpu.matmul_pop(acc[q][s])

        for part in range(1, tp_size):
            w_in_pad_ref[:latent_dims, :] = w_in_refs[part - 1][...]
            w_in_pad_ref[latent_dims:, :] = jnp.zeros(
                (TILE - latent_dims, units), jnp.bfloat16
            )
            for tile in range(0, units // TILE, 2):
                for q in range(2):
                    at = (tile + q) * TILE
                    pltpu.matmul_push_rhs(
                        w_in_pad_ref[:, at : at + TILE], staging_register=1, mxu_index=q
                    )
                for s in range(samples):
                    for q in range(2):
                        pltpu.matmul_acc_lhs(
                            acc[q][s],
                            latent_ref[rows[s], :],
                            load_staged_rhs=1 if s == 0 else None,
                        )
                for s in range(samples):
                    for q in range(2):
                        at = (tile + q) * TILE
                        bias = b_in_refs[part - 1][:, at : at + TILE].astype(jnp.float32)
                        unit = jnp.maximum(pltpu.matmul_pop(acc[q][s]) + bias, 0.0)
                        at += (part - 1) * units
                        hidden_ref[rows[s], at : at + TILE] = unit.astype(jnp.bfloat16)

        def lhs(s, k):
            at = k * TILE
            if at < units:
                return own_ref[rows[s], at : at + TILE]
            return hidden_ref[rows[s], at - units : at - units + TILE]

        def in_head(block):
            return isinstance(block, int) and block < heads

        def push(block, k):
            for q in range(2):
                deep, wide = slice(k * TILE, (k + 1) * TILE), slice(q * TILE, (q + 1) * TILE)
                if in_head(block):
                    tile = head_ref[block, deep, wide]
                else:
                    tile = w_ref[block - heads, deep, wide]
                pltpu.matmul_push_rhs(tile, staging_register=k % 2, mxu_index=q)

        def columns_of(block, first_column, count):
            at = block * width + first_column
            return pl.ds(at if isinstance(block, int) else pl.multiple_of(at, count), count)

        def make_target(block):
            columns = columns_of(block, 0, width)
            image = image_ref[:, columns].astype(jnp.float32)
            target_ref[block] = (image - bias_ref[:, columns]) * inverse_ref[:1, columns]

        def finish_row(s, total):
            lanes = jnp.sum(total.T, axis=0, keepdims=True)
            row_ref[s : s + 1, :] = prior_ref[s : s + 1, :] - 0.5 * lanes

        def take(block, s):
            total = squares_ref[s]
            for q in range(2):
                product = pltpu.matmul_pop(acc[q][s]).reshape(images // 8, 8, TILE)
                inverse = inverse_ref[:, columns_of(block, q * TILE, TILE)]
                wide = slice(q * TILE, (q + 1) * TILE)
                target = target_ref[block, :, wide]
                scaled = target.reshape(images // 8, 8, TILE) - product * inverse[None]
                square = (scaled * scaled).reshape(images, TILE)
                for lane in range(0, TILE, LANES):
                    total = total + square[:, lane : lane + LANES]
            if isinstance(block, int) and block == blocks - 1:
                finish_row(s, total)
            else:
                squares_ref[s] = total

        middle = depth // 2
        first, second = range(samples // 2), range(samples // 2, samples)

        def multiply(block, mine, depths, following, taken, done):
            for k in depths:
                for index, s in enumerate(mine):
                    for q in range(2):
                        pltpu.matmul_acc_lhs(
                            acc[q][s], lhs(s, k), load_staged_rhs=k % 2 if index == 0 else None
                        )
                    if index == 0:
                        if k + 1 < depth:
                            push(block, k + 1)
                        else:
                            push(following, 0)
                count = len(done)
                for s in done[k * count // depth : (k + 1) * count // depth]:
                    take(taken, s)

        def block_step(block):
            if not in_head(block + 1):
                for copy in fetches(block + 1):
                    copy.wait()
                following = block + 1 + AHEAD
                if isinstance(block, int):
                    if following < blocks:
                        start(following)
                else:
                    pl.when(following < blocks)(functools.partial(start, following))
            make_target(block + 1)
            multiply(block, second, range(middle, depth), block + 1, block, first)
            multiply(block + 1, first, range(depth), block + 1, block, second)
            multiply(block + 1, second, range(middle), None, block + 1, first)

        squares_ref[...] = jnp.zeros_like(squares_ref)
        push(0, 0)
        make_target(0)
        multiply(0, first, range(depth), 0, 0, ())
        multiply(0, second, range(middle), None, 0, first)
        for block in range(heads):
            block_step(block)

        @pl.loop(heads, blocks - 1)
        def _(block):
            block_step(block)

        last = blocks - 1
        done = middle * len(first) // depth
        left = first[done:]
        for index, s in enumerate(second):
            for k in range(middle, depth):
                for q in range(2):
                    pltpu.matmul_acc_lhs(acc[q][s], lhs(s, k), load_staged_rhs=k % 2)
                if k + 1 < depth:
                    push(last, k + 1)
                elif s != second[-1]:
                    push(last, middle)
            if index < len(left):
                take(last, left[index])
            if index > 0:
                take(last, second[index - 1])
        for s in first[:done]:
            finish_row(s, squares_ref[s])
        take(last, second[-1])
        out_ref[...] = jnp.broadcast_to(row_ref[...][None], out_ref.shape)

    pl.run_scoped(
        body,
        *[
            pltpu.ACC(q)((images, TILE), jnp.float32)
            for q in range(2)
            for _ in range(samples)
        ],
    )


def finish_kernel(samp_axis, tp_size, all_pixels, received_ref, bound_ref, weights_ref):
    samp_size = received_ref.shape[0] // tp_size
    samples = received_ref.shape[1]
    all_samples = samp_size * samples
    parts = received_ref[...].reshape(samp_size, tp_size, *received_ref.shape[1:])
    logw = parts[:, 0]
    for half in range(1, tp_size):
        logw = logw + parts[:, half]
    peak = jnp.max(jnp.max(logw, axis=0), axis=0, keepdims=True)
    sum_exp = jnp.sum(jnp.sum(jnp.exp(logw - peak[None]), axis=0), axis=0, keepdims=True)
    log_sum = jnp.log(sum_exp)
    log_count = math.log(all_samples)
    bound_ref[...] = (peak + log_sum - log_count) / all_pixels
    me = lax.axis_index(samp_axis)
    own = received_ref[pl.ds(me * tp_size, tp_size)]
    mine = own[0]
    for half in range(1, tp_size):
        mine = mine + own[half]
    weights_ref[...] = (mine - peak) - log_sum + log_count


def on_device(
    mesh_shape, images, enc_mean, enc_logscale, noise, w_in, b_in, w_out, b_out, pixel_logscale
):
    samp_size, tp_size = mesh_shape["samp"], mesh_shape["tp"]
    devices = samp_size * tp_size
    image_count, sample_count, latent_dims = noise.shape
    rows = image_count * sample_count
    units = w_in.shape[1]
    hidden_units, pixels = w_out.shape
    width = 2 * TILE
    blocks = pixels // width
    heads = min(2, blocks - 1)

    def from_neighbour(value, shift):
        return lax.ppermute(
            value, "tp", [(a, (a + shift) % tp_size) for a in range(tp_size)]
        )

    w_in_others = [from_neighbour(w_in, shift) for shift in range(1, tp_size)]
    b_in_others = [from_neighbour(b_in, shift) for shift in range(1, tp_size)]
    hbm = pl.BlockSpec(memory_space=pltpu.HBM)
    vmem = pl.BlockSpec(memory_space=pltpu.VMEM)
    f32, bf16 = jnp.float32, jnp.bfloat16
    in_hbm = lambda value: pltpu.with_memory_space_constraint(value, pltpu.HBM)
    prepared = pl.pallas_call(
        functools.partial(prepare_kernel, "tp", tp_size),
        in_specs=[hbm] * 7,
        out_specs=[vmem] * 5,
        out_shape=[
            jax.ShapeDtypeStruct((rows, TILE), bf16),
            jax.ShapeDtypeStruct((rows, units), bf16),
            jax.ShapeDtypeStruct((sample_count, image_count), f32),
            jax.ShapeDtypeStruct((8, pixels), f32),
            jax.ShapeDtypeStruct((heads, hidden_units, width), bf16),
        ],
        scratch_shapes=[
            pltpu.VMEM((sample_count, image_count, latent_dims), f32),
            pltpu.VMEM(enc_mean.shape, f32),
            pltpu.VMEM(enc_logscale.shape, f32),
            pltpu.VMEM(w_in.shape, bf16),
            pltpu.VMEM(b_in.shape, bf16),
            pltpu.VMEM(pixel_logscale.shape, f32),
            pltpu.SemaphoreType.DMA((sample_count + 5,)),
            pltpu.SemaphoreType.DMA((heads, tp_size)),
        ],
        compiler_params=pltpu.CompilerParams(vmem_limit_bytes=14 << 20),
        cost_estimate=pl.CostEstimate(
            flops=2 * rows * latent_dims * units + 20 * image_count * pixels,
            bytes_accessed=2 * image_count * pixels + 4 * rows * latent_dims,
            transcendentals=pixels,
        ),
        name="prepare",
    )(*map(in_hbm, (noise, enc_mean, enc_logscale, w_in, b_in, pixel_logscale, w_out)))
    partial = pl.pallas_call(
        functools.partial(decoder_kernel, "tp", tp_size),
        in_specs=[vmem] * (7 + 2 * (tp_size - 1)) + [hbm],
        out_specs=vmem,
        out_shape=jax.ShapeDtypeStruct((devices, sample_count, image_count), f32),
        scratch_shapes=[
            pltpu.VMEM((rows, hidden_units - units), bf16),
            pltpu.VMEM((blocks - heads, hidden_units, width), bf16),
            pltpu.VMEM((blocks, image_count, width), f32),
            pltpu.VMEM((sample_count, image_count, LANES), f32),
            pltpu.VMEM((sample_count, image_count), f32),
            pltpu.VMEM((TILE, units), bf16),
            pltpu.SemaphoreType.DMA((blocks - heads, tp_size)),
        ],
        compiler_params=pltpu.CompilerParams(vmem_limit_bytes=32 << 20),
        cost_estimate=pl.CostEstimate(
            flops=2 * rows * hidden_units * pixels,
            bytes_accessed=2 * hidden_units * pixels,
            transcendentals=0,
        ),
        name="decoder",
    )(*prepared[:4], b_out, prepared[4], *w_in_others, *b_in_others, images, in_hbm(w_out))
    received = lax.all_to_all(partial, ("samp", "tp"), 0, 0)
    bound, weights = pl.pallas_call(
        functools.partial(finish_kernel, "samp", tp_size, pixels * tp_size),
        in_specs=[vmem],
        out_shape=(
            jax.ShapeDtypeStruct((1, image_count), f32),
            jax.ShapeDtypeStruct((sample_count, image_count), f32),
        ),
        compiler_params=pltpu.CompilerParams(vmem_limit_bytes=4 << 20),
        name="finish",
    )(received)
    return bound.reshape(image_count), weights.T


def solution(mesh):
    in_specs = (
        P(None, "tp"),
        P(),
        P(),
        P(None, "samp", None),
        P(None, "tp"),
        P(None, "tp"),
        P(None, "tp"),
        P(None, "tp"),
        P(None, "tp"),
    )
    out_specs = (P(), P(None, "samp"))
    return jax.shard_map(
        functools.partial(on_device, dict(mesh.shape)),
        mesh=mesh,
        in_specs=in_specs,
        out_specs=out_specs,
        check_vma=False,
    )
```
